32 devices in a mesh: shift: 2 (over x), batch: 4 (over z), cols: 4 (over y, core).
Axes of the slice: x: 2, y: 2, z: 4, core: 2. Of those that a mesh axis runs over, the one named last changes fastest.
Arguments:
- partial_up: float32 [8, 768, 3072], P(('shift', 'batch'), None, 'cols'), parts along dimension 0, may hold values from -0.875 to 0.875
- partial_down: float32 [8, 3072, 768], P(('shift', 'batch'), 'cols'), parts along dimension 0, may hold values from -0.875 to 0.875
- partial_norm: float32 [8, 768], P(('shift', 'batch')), parts along dimension 0, may hold values from -8 to 8
- partial_bias: float32 [8, 768], P(('shift', 'batch')), parts along dimension 0, may hold values from -8 to 8
- master_up: float32 [1536, 3072], P(('shift', 'batch'), 'cols'), parts along dimension 0, may hold values from -0.21875 to 0.21875
- master_down: float32 [6144, 768], P(('shift', 'cols'), 'batch'), parts along dimension 0, may hold values from -0.109375 to 0.109375
- master_norm: float32 [1536], P(('shift', 'batch')), parts along dimension 0, may hold values from 0.25 to 1.75
- master_bias: float32 [1536], P(('shift', 'batch')), parts along dimension 0, may hold values from -3 to 3
- memory_up: float32 [1536, 3072], P(('shift', 'batch'), 'cols'), parts along dimension 0, may hold values from -1.75 to 1.75
- memory_down: float32 [6144, 768], P(('shift', 'cols'), 'batch'), parts along dimension 0, may hold values from -1.75 to 1.75
- memory_norm: float32 [1536], P(('shift', 'batch')), parts along dimension 0, may hold values from -1.75 to 1.75
- memory_bias: float32 [1536], P(('shift', 'batch')), parts along dimension 0, may hold values from -1.75 to 1.75
Outputs:
- compute_up: bfloat16 [1536, 3072], P('shift', 'cols'), parts along dimension 0
- compute_down: bfloat16 [6144, 768], P(('shift', 'cols')), parts along dimension 0
- compute_norm: bfloat16 [1536], P('shift'), parts along dimension 0
- compute_bias: bfloat16 [1536], P('shift'), parts along dimension 0
- stepped_up: float32 [1536, 3072], P(('shift', 'batch'), 'cols'), parts along dimension 0
- stepped_down: float32 [6144, 768], P(('shift', 'cols'), 'batch'), parts along dimension 0
- stepped_norm: float32 [1536], P(('shift', 'batch')), parts along dimension 0
- stepped_bias: float32 [1536], P(('shift', 'batch')), parts along dimension 0
- state_new_up: float32 [1536, 3072], P(('shift', 'batch'), 'cols'), parts along dimension 0
- state_new_down: float32 [6144, 768], P(('shift', 'cols'), 'batch'), parts along dimension 0
- state_new_norm: float32 [1536], P(('shift', 'batch')), parts along dimension 0
- state_new_bias: float32 [1536], P(('shift', 'batch')), parts along dimension 0
The draws below stay inside these ranges and needn't reach their ends.
There are 2 independent parts, one for each index of `shift`. The reference program is written for one: setup_inputs(seed, part) draws one part's arguments, and reference() takes and returns one part's arrays. A program takes and returns all parts, laid end to end along the dimension named above; each array names one. Nothing has to cross between parts.
All inputs are finite; a program needn't handle non-finite values.
Results may differ from the reference program's by a relative error of at most 0.0085.
Values may be sent and summed in bfloat16 or wider, within the bound.
A program may use at most 64 MiB of HBM per device.

```python
import jax
import jax.numpy as jnp

WIDTH = 768
INNER = 3072
REPLICAS = 4


def raised(drawn, rng, source, target, parts, factor):
    def block_of(position):
        return (jnp.arange(drawn.shape[position]) // (drawn.shape[position] // parts)).reshape((-1,) + (1,) * (drawn.ndim - 1 - position))

    first = jax.random.permutation(rng, parts)[block_of(target)]
    second = (block_of(target) + parts // 2) % parts
    return jnp.where((block_of(source) == first) | (block_of(source) == second), factor * drawn, drawn)


def block_scale(key, shape, shards, low, largest):
    def one(position, parts):
        steps = jax.random.uniform(jax.random.fold_in(jax.random.fold_in(key, 6), position), (parts,), jnp.float32, low / len(shards), largest / len(shards))
        return jnp.repeat(jnp.exp(steps), shape[position] // parts).reshape((-1,) + (1,) * (len(shape) - position - 1))

    level = one(*shards[0])
    for cut in shards[1:]:
        level = level * one(*cut)
    return level


def noise(rng, shape, deviation, reach, pieces=(), held_as=jnp.bfloat16):
    drawn = deviation * jax.random.normal(rng, shape, jnp.float32)
    if pieces:
        drawn = drawn * block_scale(rng, shape, pieces, -0.22, 0.18)
    return jnp.clip(drawn, -reach, reach).astype(held_as)


def noise_with(key, shape, scale, most, split, heavy, dtype=jnp.bfloat16):
    values = scale * jax.random.normal(key, shape, jnp.float32)
    if split:
        values = values * block_scale(key, shape, split, -0.22, 0.18)
    return jnp.clip(raised(values, jax.random.fold_in(key, 3), *heavy), -most, most).astype(dtype)


def setup_inputs(seed: int = 0, part: int = 0) -> dict:
    arg_keys = jax.random.split(jax.random.key(seed), 13)
    part_keys = jax.random.split(jax.random.fold_in(arg_keys[12], part), 13)
    return {
        "partial_up": noise_with(part_keys[0], (REPLICAS, WIDTH, INNER), 0.1, 0.875, ((0, 4), (2, 4)), (0, 1, 4, 2.0), jnp.float32),
        "partial_down": noise_with(part_keys[1], (REPLICAS, INNER, WIDTH), 0.1, 0.875, ((0, 4), (1, 4)), (0, 2, 4, 2.0), jnp.float32),
        "partial_norm": noise_with(part_keys[2], (REPLICAS, WIDTH), 1.0, 8.0, ((0, 4),), (0, 1, 4, 2.0), jnp.float32),
        "partial_bias": noise_with(part_keys[3], (REPLICAS, WIDTH), 1.0, 8.0, ((0, 4),), (0, 1, 4, 2.0), jnp.float32),
        "master_up": noise(part_keys[4], (WIDTH, INNER), WIDTH ** -0.5, 0.21875, ((0, 4), (1, 4)), jnp.float32),
        "master_down": noise(part_keys[5], (INNER, WIDTH), INNER ** -0.5, 0.109375, ((0, 4), (1, 4)), jnp.float32),
        "master_norm": jnp.clip(1.0 + 0.15 * jax.random.normal(part_keys[6], (WIDTH,), jnp.float32), 0.25, 1.75),
        "master_bias": noise(part_keys[7], (WIDTH,), 0.5, 3.0, ((0, 4),), jnp.float32),
        "memory_up": noise(part_keys[8], (WIDTH, INNER), 0.3, 1.75, ((0, 4), (1, 4)), jnp.float32),
        "memory_down": noise(part_keys[9], (INNER, WIDTH), 0.3, 1.75, ((0, 4), (1, 4)), jnp.float32),
        "memory_norm": noise(part_keys[10], (WIDTH,), 0.3, 1.75, ((0, 4),), jnp.float32),
        "memory_bias": noise(part_keys[11], (WIDTH,), 0.3, 1.75, ((0, 4),), jnp.float32),
    }


learn_rate = 0.1
hold_rate = 0.8


def reference(partial_up, partial_down, partial_norm, partial_bias, master_up, master_down, master_norm, master_bias, memory_up, memory_down, memory_norm, memory_bias):
    mean_up = jnp.sum(partial_up.astype(jnp.float32), axis=0) * REPLICAS ** -0.5
    mean_down = jnp.sum(partial_down.astype(jnp.float32), axis=0) * REPLICAS ** -0.5
    mean_norm = jnp.sum(partial_norm.astype(jnp.float32), axis=0) * REPLICAS ** -0.5
    mean_bias = jnp.sum(partial_bias.astype(jnp.float32), axis=0) * REPLICAS ** -0.5
    state_new_up = hold_rate * memory_up + mean_up
    stepped_up = master_up - learn_rate * state_new_up
    state_new_down = hold_rate * memory_down + mean_down
    stepped_down = master_down - learn_rate * state_new_down
    state_new_norm = hold_rate * memory_norm + mean_norm
    stepped_norm = master_norm - learn_rate * state_new_norm
    state_new_bias = hold_rate * memory_bias + mean_bias
    stepped_bias = master_bias - learn_rate * state_new_bias
    compute_up = stepped_up.astype(jnp.bfloat16)
    compute_down = stepped_down.astype(jnp.bfloat16)
    compute_norm = stepped_norm.astype(jnp.bfloat16)
    compute_bias = stepped_bias.astype(jnp.bfloat16)
    return compute_up, compute_down, compute_norm, compute_bias, stepped_up, stepped_down, stepped_norm, stepped_bias, state_new_up, state_new_down, state_new_norm, state_new_bias
```

```python
import functools

import jax
import jax.numpy as jnp
from jax import lax
from jax.experimental import pallas as pl
from jax.experimental.pallas import tpu as pltpu
from jax.sharding import PartitionSpec as P

learn_rate = 0.1
hold_rate = 0.8
bf16, f32 = jnp.bfloat16, jnp.float32
MESH = pl.DeviceIdType.MESH
RIGHT, LEFT = 0, 1


def kernel(
    n, rate,
    pu, pd, pn, pb, mu, md, mn, mb, hu, hd, hn, hb,
    cu, cd, cv, su, sd, sv, tu, td, tv,
    vpu, vpd, vmu, vmd, vhu, vhd, send, got, res, vs, vr, vg,
    in_sem, rs_send, rs_recv, ag_send, ag_recv, vec_send, vec_recv,
):
    me = lax.axis_index("batch")
    rows = vpu.shape[0]
    w = rows // n
    half = vpu.shape[1] // 2
    p = half // w
    far = n // 2
    toward = ({"batch": lax.rem(me + 1, n)}, {"batch": lax.rem(me + n - 1, n)})

    def at(d):
        return lax.rem(me + d + n, n)

    def block(side, d):
        return at(d) if side == RIGHT else at(-d)

    def reach(side, q):
        return far if q % 2 == side else far - 1

    loads = {}

    def load(name, src, dst):
        copy = pltpu.make_async_copy(src, dst, in_sem.at[len(loads)])
        copy.start()
        loads[name] = copy

    order = [d for d in (far, *(s * e for e in range(far - 1, 0, -1) for s in (1, -1)), 0)]
    for d in order:
        r = pl.ds(pl.multiple_of(at(d) * w, w), w)
        load(("up", d), pu.at[0, r, :], vpu.at[r, :])
    for h in range(2):
        r = pl.ds(h * (rows // 2), rows // 2)
        load(("down", h), pd.at[0, r, :], vpd.at[r, :])
    load("mu", mu, vmu)
    load("hu", hu, vhu)
    load("md", md, vmd)
    load("hd", hd, vhd)

    barrier = pltpu.get_barrier_semaphore()
    for d in range(1, n):
        pl.semaphore_signal(barrier, inc=1, device_id={"batch": at(d)}, device_id_type=MESH)

    def pack_up(d):
        loads["up", d].wait()
        r = pl.ds(pl.multiple_of(at(d) * w, w), w)
        for h in range(2):
            send[at(d), h] = vpu[r, h * half : (h + 1) * half].astype(bf16)

    def pack_down(h):
        loads["down", h].wait()
        for k in range(n):
            send[k, 2 + h] = jnp.concatenate(
                [
                    vpd[(h * p + g) * w : (h * p + g + 1) * w, k * w : (k + 1) * w]
                    for g in range(p)
                ],
                axis=1,
            ).astype(bf16)

    def scatter(side, q, d):
        return pltpu.make_async_remote_copy(
            src_ref=send.at[block(side, d), q],
            dst_ref=got.at[side, q, d - 1],
            send_sem=rs_send.at[side, q, d - 1],
            recv_sem=rs_recv.at[side, q, d - 1],
            device_id=toward[side],
            device_id_type=MESH,
        )

    def gather(side, q, d):
        origin = block(side, -(d - 1))
        return pltpu.make_async_remote_copy(
            src_ref=res.at[origin, q],
            dst_ref=res.at[origin, q],
            send_sem=ag_send.at[side, q, d - 1],
            recv_sem=ag_recv.at[side, q, d - 1],
            device_id=toward[side],
            device_id_type=MESH,
        )

    def arriving(side, q, d):
        origin = block(side, -d)
        return pltpu.make_async_remote_copy(
            src_ref=res.at[origin, q],
            dst_ref=res.at[origin, q],
            send_sem=ag_send.at[side, q, d - 1],
            recv_sem=ag_recv.at[side, q, d - 1],
            device_id=toward[side],
            device_id_type=MESH,
        )

    def vector(phase, d, src, dst):
        return pltpu.make_async_remote_copy(
            src_ref=src,
            dst_ref=dst,
            send_sem=vec_send.at[phase, d],
            recv_sem=vec_recv.at[phase, d],
            device_id={"batch": at(d)},
            device_id_type=MESH,
        )

    def step(q, d):
        for side in sorted((RIGHT, LEFT), key=lambda s: d < reach(s, q)):
            if d > reach(side, q):
                continue
            if d < reach(side, q):
                scatter(side, q, d + 1).wait_recv()
                b = block(side, d)
                send[b, q] = (send[b, q].astype(f32) + got[side, q, d].astype(f32)).astype(bf16)
            scatter(side, q, d).start()

    pack_up(far)
    pl.semaphore_wait(barrier, n - 1)
    for h in range(2):
        step(h, far)
    for h in range(2):
        pack_down(h)
        step(2 + h, far)
    for k in range(n):
        vs[k, 0:1, :] = pn[:, k * w : (k + 1) * w]
        vs[k, 1:2, :] = pb[:, k * w : (k + 1) * w]
    for d in range(1, n):
        vector(0, d, vs.at[at(d)], vr.at[d]).start()
    for d in range(far - 1, 0, -1):
        pack_up(d)
        pack_up(-d)
        for q in range(4):
            step(q, d)
    pack_up(0)

    total = vs[me]
    for d in range(1, n):
        vector(0, d, vs.at[at(d)], vr.at[d]).wait_recv()
        total = total + vr[d]
    for i, (m, h) in enumerate(((mn, hn), (mb, hb))):
        state = hold_rate * h[...] + total[i : i + 1] * rate
        stepped = m[...] - learn_rate * state
        tv[i : i + 1, :] = state
        sv[i : i + 1, :] = stepped
        vg[me, i : i + 1, :] = stepped
    for d in range(1, n):
        vector(1, d, vg.at[me], vg.at[me]).start()

    def total_of(q):
        total = send[me, q].astype(f32)
        for side in (RIGHT, LEFT):
            if reach(side, q) >= 1:
                scatter(side, q, 1).wait_recv()
                total = total + got[side, q, 0].astype(f32)
        return total * rate

    def publish(q):
        for side in (RIGHT, LEFT):
            if reach(side, q) >= 1:
                gather(side, q, 1).start()

    loads["mu"].wait()
    loads["hu"].wait()
    for h in range(2):
        lanes = slice(h * half, (h + 1) * half)
        state = hold_rate * vhu[:, lanes] + total_of(h)
        stepped = vmu[:, lanes] - learn_rate * state
        res[me, h] = stepped.astype(bf16)
        publish(h)
        tu[:, lanes] = state
        su[:, lanes] = stepped
    loads["md"].wait()
    loads["hd"].wait()
    for h in range(2):
        total = total_of(2 + h)
        parts = []
        for g in range(p):
            r = slice((h * p + g) * w, (h * p + g + 1) * w)
            state = hold_rate * vhd[r, :] + total[:, g * w : (g + 1) * w]
            stepped = vmd[r, :] - learn_rate * state
            td[r, :] = state
            sd[r, :] = stepped
            parts.append(stepped)
        res[me, 2 + h] = jnp.concatenate(parts, axis=1).astype(bf16)
        publish(2 + h)

    def place_up(d, q):
        r = pl.ds(pl.multiple_of(at(d) * w, w), w)
        cu[r, q * half : (q + 1) * half] = res[at(d), q]

    for q in range(2):
        place_up(0, q)
    for d in range(1, far + 1):
        for q in range(4):
            for side in (RIGHT, LEFT):
                if d <= reach(side, q):
                    arriving(side, q, d).wait_recv()
                    if d + 1 <= reach(side, q):
                        gather(side, q, d + 1).start()
                    if q < 2:
                        place_up(-d if side == RIGHT else d, q)
        if d == 1:
            for e in range(1, n):
                vector(1, e, vg.at[at(-e)], vg.at[at(-e)]).wait_recv()
            for k in range(n):
                cv[:, k * w : (k + 1) * w] = vg[k]
    for h in range(2):
        for g in range(p):
            cd[(h * p + g) * w : (h * p + g + 1) * w, :] = jnp.concatenate(
                [res[k, 2 + h, :, g * w : (g + 1) * w].astype(f32) for k in range(n)], axis=1
            ).astype(bf16)

    for side in (RIGHT, LEFT):
        for q in range(4):
            for d in range(1, reach(side, q) + 1):
                scatter(side, q, d).wait_send()
                gather(side, q, d).wait_send()
    for d in range(1, n):
        vector(0, d, vs.at[at(d)], vr.at[d]).wait_send()
        vector(1, d, vg.at[me], vg.at[me]).wait_send()


def on_device(pu, pd, pn, pb, mu, md, mn, mb, hu, hd, hn, hb):
    n = lax.axis_size("batch")
    rows, columns = pu.shape[1:]
    w = rows // n
    half = columns // 2
    far = n // 2
    line = lambda v: v.reshape(1, -1)
    shape = jax.ShapeDtypeStruct
    vmem = pl.BlockSpec(memory_space=pltpu.VMEM)
    hbm = pl.BlockSpec(memory_space=pl.ANY)
    kinds = (hbm, hbm, vmem, vmem) + (hbm, hbm, vmem, vmem) * 2
    dma = pltpu.SemaphoreType.DMA
    cu, cd, cv, su, sd, sv, tu, td, tv = pl.pallas_call(
        functools.partial(kernel, n, n ** (-0.5)),
        out_shape=(
            shape((rows, columns), bf16),
            shape(pd.shape[1:], bf16),
            shape((2, rows), f32),
            shape(mu.shape, f32),
            shape(md.shape, f32),
            shape((2, w), f32),
            shape(mu.shape, f32),
            shape(md.shape, f32),
            shape((2, w), f32),
        ),
        in_specs=kinds,
        out_specs=(vmem,) * 9,
        scratch_shapes=[
            pltpu.VMEM(pu.shape[1:], f32),
            pltpu.VMEM(pd.shape[1:], f32),
            pltpu.VMEM(mu.shape, f32),
            pltpu.VMEM(md.shape, f32),
            pltpu.VMEM(hu.shape, f32),
            pltpu.VMEM(hd.shape, f32),
            pltpu.VMEM((n, 4, w, half), bf16),
            pltpu.VMEM((2, 4, far, w, half), bf16),
            pltpu.VMEM((n, 4, w, half), bf16),
            pltpu.VMEM((n, 2, w), f32),
            pltpu.VMEM((n, 2, w), f32),
            pltpu.VMEM((n, 2, w), f32),
            dma((n + 6,)),
            dma((2, 4, far)),
            dma((2, 4, far)),
            dma((2, 4, far)),
            dma((2, 4, far)),
            dma((2, n)),
            dma((2, n)),
        ],
        compiler_params=pltpu.CompilerParams(
            collective_id=0, has_side_effects=True, vmem_limit_bytes=40 * 2**20
        ),
    )(pu, pd, pn, pb, mu, md, line(mn), line(mb), hu, hd, line(hn), line(hb))
    return (
        cu, cd, cv[0].astype(bf16), cv[1].astype(bf16),
        su, sd, sv[0], sv[1],
        tu, td, tv[0], tv[1],
    )


def solution(mesh):
    own = (
        P(("shift", "batch"), "cols"),
        P(("shift", "cols"), "batch"),
        P(("shift", "batch")),
        P(("shift", "batch")),
    )
    return jax.shard_map(
        on_device,
        mesh=mesh,
        in_specs=(
            P(("shift", "batch"), None, "cols"),
            P(("shift", "batch"), "cols", None),
            P(("shift", "batch"), None),
            P(("shift", "batch"), None),
            *own,
            *own,
        ),
        out_specs=(
            P("shift", "cols"),
            P(("shift", "cols"), None),
            P("shift"),
            P("shift"),
            *own,
            *own,
        ),
        check_vma=False,
    )
```

```python
import functools

import jax
import jax.numpy as jnp
from jax import lax
from jax.experimental import pallas as pl
from jax.experimental.pallas import tpu as pltpu
from jax.sharding import PartitionSpec as P

learn_rate = 0.1
hold_rate = 0.8
bf16, f32 = jnp.bfloat16, jnp.float32
MESH = pl.DeviceIdType.MESH
RIGHT, LEFT = 0, 1
CHUNK = 256
MOST = 67043328
LEAD = 1
LAG = 1


def line_kernel(
    n, rate,
    pu, pd, pn, pb, mu, md, mn, mb, hu, hd, hn, hb,
    cu, cd, cn, cb, su, sd, sn, sb, tu, td, tn, tb,
    vpu, vpd, vmu, vmd, vhu, vhd, vpn, vpb, vmn, vmb, vhn, vhb,
    send, got, acc, vs, vr, vg,
    in_sem, rs_send, rs_recv, ag_send, ag_recv, vec_send, vec_recv,
):
    me = lax.axis_index("batch")
    size, width = vpu.shape
    w = size // n
    per = width // CHUNK
    count = 2 * per
    first, last = me == 0, me == n - 1
    mine = pl.ds(pl.multiple_of(me * w, w), w)
    toward = ({"batch": jnp.minimum(me + 1, n - 1)}, {"batch": jnp.maximum(me - 1, 0)})

    loads = {}

    def load(name, src, dst):
        copy = pltpu.make_async_copy(src, dst, in_sem.at[len(loads)])
        copy.start()
        loads[name] = copy

    def lanes(q):
        return slice((q % per) * CHUNK, (q % per + 1) * CHUNK)

    def load_chunk(q):
        if q < per:
            load(q, pu.at[0, :, lanes(q)], vpu.at[:, lanes(q)])
        else:
            load(q, pd.at[0, lanes(q), :], vpd.at[lanes(q), :])

    for q in range(2):
        load_chunk(q)
    vectors = ((pn, vpn), (pb, vpb), (mn, vmn), (mb, vmb), (hn, vhn), (hb, vhb))
    for i, (src, dst) in enumerate(vectors):
        load(("vector", i), src, dst)
    load("mu", mu, vmu)
    load("hu", hu, vhu)
    for q in range(2, count):
        load_chunk(q)
    load("md", md, vmd)
    load("hd", hd, vhd)

    def at(d):
        return lax.rem(me + d + n, n)

    barrier = pltpu.get_barrier_semaphore()
    for d in range(1, n):
        pl.semaphore_signal(barrier, inc=1, device_id={"batch": at(d)}, device_id_type=MESH)

    def pack(q):
        loads[q].wait()
        if q < per:
            send[0, :, lanes(q)] = vpu[:, lanes(q)].astype(bf16)
        else:
            send[1, :, lanes(q)] = vpd[lanes(q), :].T.astype(bf16)

    def scatter(side, q, j):
        here = (q // per, slice(j * w, (j + 1) * w), lanes(q))
        return pltpu.make_async_remote_copy(
            src_ref=send.at[here],
            dst_ref=got.at[(side, *here)],
            send_sem=rs_send.at[side, q, j],
            recv_sem=rs_recv.at[side, q, j],
            device_id=toward[side],
            device_id_type=MESH,
        )

    def gather(side, q, j):
        out = (cu, cd)[q // per].at[pl.ds(pl.multiple_of(j * w, w), w), lanes(q)]
        return pltpu.make_async_remote_copy(
            src_ref=out,
            dst_ref=out,
            send_sem=ag_send.at[side, q, j],
            recv_sem=ag_recv.at[side, q, j],
            device_id=toward[side],
            device_id_type=MESH,
        )

    def vector(phase, d, src, dst):
        return pltpu.make_async_remote_copy(
            src_ref=src,
            dst_ref=dst,
            send_sem=vec_send.at[phase, d],
            recv_sem=vec_recv.at[phase, d],
            device_id={"batch": at(d)},
            device_id_type=MESH,
        )

    def add(side, q, j):
        here = (q // per, slice(j * w, (j + 1) * w), lanes(q))
        send[here] = (send[here].astype(f32) + got[(side, *here)].astype(f32)).astype(bf16)

    def start_ends(q):
        @pl.when(first)
        def _():
            for j in range(n - 1, 0, -1):
                scatter(RIGHT, q, j).start()

        @pl.when(last)
        def _():
            for j in range(n - 1):
                scatter(LEFT, q, j).start()

    def reduce(q):
        for s in range(n - 1):
            j = n - 1 - s

            @pl.when(jnp.logical_and(me > 0, me <= j))
            def _():
                scatter(RIGHT, q, j).wait_recv()

            @pl.when(jnp.logical_and(me > 0, me < j))
            def _():
                add(RIGHT, q, j)
                scatter(RIGHT, q, j).start()

            @pl.when(jnp.logical_and(me < n - 1, me >= s))
            def _():
                scatter(LEFT, q, s).wait_recv()

            @pl.when(jnp.logical_and(me < n - 1, me > s))
            def _():
                add(LEFT, q, s)
                scatter(LEFT, q, s).start()

    def update(q):
        m, cut = q // per, lanes(q)
        acc[...] = send[m, mine, cut].astype(f32)

        @pl.when(me > 0)
        def _():
            acc[...] += got[RIGHT, m, mine, cut].astype(f32)

        @pl.when(me < n - 1)
        def _():
            acc[...] += got[LEFT, m, mine, cut].astype(f32)

        if q % per == 0:
            loads[("mu", "md")[m]].wait()
            loads[("hu", "hd")[m]].wait()
        state = hold_rate * (vhu, vhd)[m][:, cut] + acc[...] * rate
        stepped = (vmu, vmd)[m][:, cut] - learn_rate * state
        (cu, cd)[m][mine, cut] = stepped.astype(bf16)

        @pl.when(me < n - 1)
        def _():
            gather(RIGHT, q, me).start()

        @pl.when(me > 0)
        def _():
            gather(LEFT, q, me).start()

        (tu, td)[m][:, cut] = state
        (su, sd)[m][:, cut] = stepped

    def forward(q):
        for e in range(1, n):
            @pl.when(me - e >= 0)
            def _():
                gather(RIGHT, q, me - e).wait_recv()

            @pl.when(jnp.logical_and(me - e >= 0, me < n - 1))
            def _():
                gather(RIGHT, q, me - e).start()

            @pl.when(me + e < n)
            def _():
                gather(LEFT, q, me + e).wait_recv()

            @pl.when(jnp.logical_and(me + e < n, me > 0))
            def _():
                gather(LEFT, q, me + e).start()

    pack(0)
    pl.semaphore_wait(barrier, n - 1)
    start_ends(0)
    for q in range(1, LEAD):
        pack(q)
        start_ends(q)
    for i in range(len(vectors)):
        loads["vector", i].wait()
    for k in range(n):
        vs[k, 0:1, :] = vpn[:, k * w : (k + 1) * w]
        vs[k, 1:2, :] = vpb[:, k * w : (k + 1) * w]
    for d in range(1, n):
        vector(0, d, vs.at[at(d)], vr.at[d]).start()

    for t in range(count + LAG):
        if t + LEAD < count:
            pack(t + LEAD)
            start_ends(t + LEAD)
        if t < count:
            reduce(t)
            update(t)
        if t == 1:
            total = vs[me]
            for d in range(1, n):
                vector(0, d, vs.at[at(d)], vr.at[d]).wait_recv()
                total = total + vr[d]
            for i, (m, h, s, o) in enumerate(((vmn, vhn, tn, sn), (vmb, vhb, tb, sb))):
                state = hold_rate * h[...] + total[i : i + 1] * rate
                stepped = m[...] - learn_rate * state
                s[...] = state
                o[...] = stepped
                vg[me, i : i + 1, :] = stepped
            for d in range(1, n):
                vector(1, d, vg.at[me], vg.at[me]).start()
        if t == 2:
            for e in range(1, n):
                vector(1, e, vg.at[at(-e)], vg.at[at(-e)]).wait_recv()
            for k in range(n):
                cn[:, k * w : (k + 1) * w] = vg[k, 0:1, :]
                cb[:, k * w : (k + 1) * w] = vg[k, 1:2, :]
        if t >= LAG:
            forward(t - LAG)

    for q in range(count):
        for j in range(n):
            @pl.when(me < j)
            def _():
                scatter(RIGHT, q, j).wait_send()

            @pl.when(me > j)
            def _():
                scatter(LEFT, q, j).wait_send()

            @pl.when(jnp.logical_and(me >= j, me < n - 1))
            def _():
                gather(RIGHT, q, j).wait_send()

            @pl.when(jnp.logical_and(me <= j, me > 0))
            def _():
                gather(LEFT, q, j).wait_send()
    for d in range(1, n):
        vector(0, d, vs.at[at(d)], vr.at[d]).wait_send()
        vector(1, d, vg.at[me], vg.at[me]).wait_send()


def write_kernel(
    cu, cd, cn, cb, su, sd, sn, sb, tu, td, tn, tb,
    ocu, ocd, ocn, ocb, osu, osd, osn, osb, otu, otd, otn, otb,
    vcd, sem,
):
    copies = [
        pltpu.make_async_copy(src, dst, sem.at[i])
        for i, (src, dst) in enumerate(((cu, ocu), (su, osu), (sd, osd), (tu, otu), (td, otd)))
    ]
    for copy in copies:
        copy.start()
    rows = vcd.shape[0]
    strip = rows // 3
    for i in range(3):
        r = slice(i * strip, (i + 1) * strip)
        vcd[r, :] = cd[:, r].astype(f32).T.astype(bf16)
        copies.append(pltpu.make_async_copy(vcd.at[r, :], ocd.at[r, :], sem.at[5 + i]))
        copies[-1].start()
    ocn[...] = cn[...].astype(bf16)
    ocb[...] = cb[...].astype(bf16)
    for src, dst in ((sn, osn), (sb, osb), (tn, otn), (tb, otb)):
        dst[...] = src[...]
    for copy in copies:
        copy.wait()


def on_device(pu, pd, pn, pb, mu, md, mn, mb, hu, hd, hn, hb):
    n = lax.axis_size("batch")
    size, width = pu.shape[1:]
    w = size // n
    count = 2 * width // CHUNK
    line = lambda v: v.reshape(1, -1)
    shape = jax.ShapeDtypeStruct
    vmem = pl.BlockSpec(memory_space=pltpu.VMEM)
    hbm = pl.BlockSpec(memory_space=pltpu.HBM)
    dma = pltpu.SemaphoreType.DMA
    whole, share = (size, width), (w, width)
    row, part = (1, size), (1, w)
    owned = (shape(share, f32), shape(share, f32), shape(part, f32), shape(part, f32))
    results = pl.pallas_call(
        functools.partial(line_kernel, n, n ** (-0.5)),
        out_shape=(
            shape(whole, bf16), shape(whole, bf16), shape(row, f32), shape(row, f32),
            *owned, *owned,
        ),
        in_specs=(hbm,) * 12,
        out_specs=(vmem,) * 12,
        scratch_shapes=[
            pltpu.VMEM(whole, f32),
            pltpu.VMEM(whole, f32),
            *[pltpu.VMEM(share, f32)] * 4,
            *[pltpu.VMEM(row, f32)] * 2,
            *[pltpu.VMEM(part, f32)] * 4,
            pltpu.VMEM((2, *whole), bf16),
            pltpu.VMEM((2, 2, *whole), bf16),
            pltpu.VMEM((w, CHUNK), f32),
            *[pltpu.VMEM((n, 2, w), f32)] * 3,
            dma((count + 10,)),
            *[dma((2, count, n))] * 4,
            *[dma((2, n))] * 2,
        ],
        compiler_params=pltpu.CompilerParams(
            collective_id=0, has_side_effects=True, vmem_limit_bytes=MOST
        ),
    )(pu, pd, pn, pb, mu, md.T, line(mn), line(mb), hu, hd.T, line(hn), line(hb))
    cu, cd, cn, cb, su, sd, sn, sb, tu, td, tn, tb = pl.pallas_call(
        write_kernel,
        out_shape=(
            shape(whole, bf16), shape(whole, bf16), shape(row, bf16), shape(row, bf16),
            *owned, *owned,
        ),
        in_specs=(vmem,) * 12,
        out_specs=(hbm, hbm, vmem, vmem) * 3,
        scratch_shapes=[pltpu.VMEM(whole, bf16), dma((8,))],
        compiler_params=pltpu.CompilerParams(vmem_limit_bytes=MOST),
    )(*results)
    flat = lambda v: v.reshape(-1)
    return (
        cu, cd, flat(cn), flat(cb),
        su, sd.T, flat(sn), flat(sb),
        tu, td.T, flat(tn), flat(tb),
    )


def solution(mesh):
    own = (
        P(("shift", "batch"), "cols"),
        P(("shift", "cols"), "batch"),
        P(("shift", "batch")),
        P(("shift", "batch")),
    )
    return jax.shard_map(
        on_device,
        mesh=mesh,
        in_specs=(
            P(("shift", "batch"), None, "cols"),
            P(("shift", "batch"), "cols", None),
            P(("shift", "batch"), None),
            P(("shift", "batch"), None),
            *own,
            *own,
        ),
        out_specs=(
            P("shift", "cols"),
            P(("shift", "cols"), None),
            P("shift"),
            P("shift"),
            *own,
            *own,
        ),
        check_vma=False,
    )
```

```python
import functools

import jax
import jax.numpy as jnp
from jax import lax
from jax.experimental import pallas as pl
from jax.experimental.pallas import tpu as pltpu
from jax.sharding import PartitionSpec as P

learn_rate = 0.1
hold_rate = 0.8
bf16, f32 = jnp.bfloat16, jnp.float32
MESH = pl.DeviceIdType.MESH
RIGHT, LEFT = 0, 1
SUBS = 3
MOST = 67043328


def line_kernel(
    n, rate,
    pu, pd, pn, pb, mu, md, mn, mb, hu, hd, hn, hb,
    cu, cd, cn, cb, su, sd, sn, sb, tu, td, tn, tb,
    vpu, vpd, vmu, vmd, vhu, vhd, vpn, vpb, vmn, vmb, vhn, vhb,
    send, got, acc, vs, vr, vg,
    in_sem, rs_send, rs_recv, ag_send, ag_recv, vec_send, vec_recv,
):
    me = lax.axis_index("batch")
    size, width = vpu.shape
    w = size // n
    per = SUBS
    count = 2 * per
    r = w // per
    first, last = me == 0, me == n - 1
    toward = ({"batch": jnp.minimum(me + 1, n - 1)}, {"batch": jnp.maximum(me - 1, 0)})

    loads = {}

    def load(name, src, dst):
        copy = pltpu.make_async_copy(src, dst, in_sem.at[len(loads)])
        copy.start()
        loads[name] = copy

    def rows(q, j):
        if isinstance(j, int):
            return pl.ds(j * w + q % per * r, r)
        return pl.ds(pl.multiple_of(j * w + q % per * r, r), r)

    def part(q):
        return pl.ds(q % per * r, r)

    def load_up(q):
        for j in range(n):
            load((q, j), pu.at[0, rows(q, j), :], vpu.at[rows(q, j), :])

    load_up(0)
    load("down", pd.at[0], vpd)
    vectors = ((pn, vpn), (pb, vpb), (mn, vmn), (mb, vmb), (hn, vhn), (hb, vhb))
    for i, (src, dst) in enumerate(vectors):
        load(("vector", i), src, dst)
    load("mu", mu, vmu)
    load("hu", hu, vhu)
    for q in range(1, per):
        load_up(q)
    load("md", md, vmd)
    load("hd", hd, vhd)

    def at(d):
        return lax.rem(me + d + n, n)

    barrier = pltpu.get_barrier_semaphore()
    for d in range(1, n):
        pl.semaphore_signal(barrier, inc=1, device_id={"batch": at(d)}, device_id_type=MESH)

    def pack(q):
        if q < per:
            for j in range(n):
                loads[q, j].wait()
                send[0, rows(q, j), :] = vpu[rows(q, j), :].astype(bf16)
        elif q == per:
            loads["down"].wait()
            strip = width // 3
            for i in range(3):
                cut = slice(i * strip, (i + 1) * strip)
                send[1, :, cut] = vpd[cut, :].T.astype(bf16)

    def scatter(side, q, j):
        here = (q // per, rows(q, j))
        return pltpu.make_async_remote_copy(
            src_ref=send.at[here],
            dst_ref=got.at[(side, *here)],
            send_sem=rs_send.at[side, q, j],
            recv_sem=rs_recv.at[side, q, j],
            device_id=toward[side],
            device_id_type=MESH,
        )

    def gather(side, q, j):
        out = (cu, cd)[q // per].at[rows(q, j)]
        return pltpu.make_async_remote_copy(
            src_ref=out,
            dst_ref=out,
            send_sem=ag_send.at[side, q, j],
            recv_sem=ag_recv.at[side, q, j],
            device_id=toward[side],
            device_id_type=MESH,
        )

    def vector(phase, d, src, dst):
        return pltpu.make_async_remote_copy(
            src_ref=src,
            dst_ref=dst,
            send_sem=vec_send.at[phase, d],
            recv_sem=vec_recv.at[phase, d],
            device_id={"batch": at(d)},
            device_id_type=MESH,
        )

    def add(side, q, j):
        here = (q // per, rows(q, j))
        send[here] = (send[here].astype(f32) + got[(side, *here)].astype(f32)).astype(bf16)

    def start_ends(q):
        @pl.when(first)
        def _():
            for j in range(n - 1, 0, -1):
                scatter(RIGHT, q, j).start()

        @pl.when(last)
        def _():
            for j in range(n - 1):
                scatter(LEFT, q, j).start()

    def reduce(side, q, i):
        blocks = range(n - 1, i - 1, -1) if side == RIGHT else range(i + 1)
        for j in blocks:
            scatter(side, q, j).wait_recv()
            if j != i:
                add(side, q, j)
                scatter(side, q, j).start()

    def update(q):
        m, own, cut = q // per, rows(q, me), part(q)
        acc[...] = send[m, own].astype(f32)

        @pl.when(me > 0)
        def _():
            acc[...] += got[RIGHT, m, own].astype(f32)

        @pl.when(me < n - 1)
        def _():
            acc[...] += got[LEFT, m, own].astype(f32)

        state = hold_rate * (vhu, vhd)[m][cut, :] + acc[...] * rate
        stepped = (vmu, vmd)[m][cut, :] - learn_rate * state
        (cu, cd)[m][own, :] = stepped.astype(bf16)

        @pl.when(me < n - 1)
        def _():
            gather(RIGHT, q, me).start()

        @pl.when(me > 0)
        def _():
            gather(LEFT, q, me).start()

        (tu, td)[m][cut, :] = state
        (su, sd)[m][cut, :] = stepped

    def forward(side, q, i, j):
        gather(side, q, j).wait_recv()
        if i != (n - 1 if side == RIGHT else 0):
            gather(side, q, j).start()

    def hop(q, d):
        for i in range(n):
            tasks = []
            if d == i > 0:
                tasks.append(functools.partial(reduce, RIGHT, q, i))
            if d == n - 1 - i > 0:
                tasks.append(functools.partial(reduce, LEFT, q, i))
            if d == max(i, n - 1 - i):
                tasks.append(functools.partial(update, q))
            for j in range(n):
                if j != i and d == max(j, n - 1 - j) + abs(i - j):
                    tasks.append(functools.partial(forward, RIGHT if j < i else LEFT, q, i, j))
            if tasks:
                @pl.when(me == i)
                def _():
                    for task in tasks:
                        task()

    pack(0)
    pl.semaphore_wait(barrier, n - 1)
    start_ends(0)
    for i in range(len(vectors)):
        loads["vector", i].wait()
    for k in range(n):
        vs[k, 0:1, :] = vpn[:, k * w : (k + 1) * w]
        vs[k, 1:2, :] = vpb[:, k * w : (k + 1) * w]
    for d in range(1, n):
        vector(0, d, vs.at[at(d)], vr.at[d]).start()

    for t in range(1, count + 2 * n - 2):
        if t < count:
            pack(t)
            start_ends(t)
        if t == 1:
            for name in ("mu", "hu", "md", "hd"):
                loads[name].wait()
        for q in range(count):
            hop(q, t - q)
        if t == 2:
            total = vs[me]
            for d in range(1, n):
                vector(0, d, vs.at[at(d)], vr.at[d]).wait_recv()
                total = total + vr[d]
            for i, (m, h, s, o) in enumerate(((vmn, vhn, tn, sn), (vmb, vhb, tb, sb))):
                state = hold_rate * h[...] + total[i : i + 1] * rate
                stepped = m[...] - learn_rate * state
                s[...] = state
                o[...] = stepped
                vg[me, i : i + 1, :] = stepped
            for d in range(1, n):
                vector(1, d, vg.at[me], vg.at[me]).start()
        if t == 3:
            for e in range(1, n):
                vector(1, e, vg.at[at(-e)], vg.at[at(-e)]).wait_recv()
            for k in range(n):
                cn[:, k * w : (k + 1) * w] = vg[k, 0:1, :]
                cb[:, k * w : (k + 1) * w] = vg[k, 1:2, :]

    for q in range(count):
        for j in range(n):
            @pl.when(me < j)
            def _():
                scatter(RIGHT, q, j).wait_send()

            @pl.when(me > j)
            def _():
                scatter(LEFT, q, j).wait_send()

            @pl.when(jnp.logical_and(me >= j, me < n - 1))
            def _():
                gather(RIGHT, q, j).wait_send()

            @pl.when(jnp.logical_and(me <= j, me > 0))
            def _():
                gather(LEFT, q, j).wait_send()
    for d in range(1, n):
        vector(0, d, vs.at[at(d)], vr.at[d]).wait_send()
        vector(1, d, vg.at[me], vg.at[me]).wait_send()


def write_kernel(
    cu, cd, cn, cb, su, sd, sn, sb, tu, td, tn, tb,
    ocu, ocd, ocn, ocb, osu, osd, osn, osb, otu, otd, otn, otb,
    vcd, sem,
):
    copies = [
        pltpu.make_async_copy(src, dst, sem.at[i])
        for i, (src, dst) in enumerate(((cu, ocu), (su, osu), (sd, osd), (tu, otu), (td, otd)))
    ]
    for copy in copies:
        copy.start()
    rows = vcd.shape[0]
    strip = rows // 3
    for i in range(3):
        r = slice(i * strip, (i + 1) * strip)
        vcd[r, :] = cd[:, r].astype(f32).T.astype(bf16)
        copies.append(pltpu.make_async_copy(vcd.at[r, :], ocd.at[r, :], sem.at[5 + i]))
        copies[-1].start()
    ocn[...] = cn[...].astype(bf16)
    ocb[...] = cb[...].astype(bf16)
    for src, dst in ((sn, osn), (sb, osb), (tn, otn), (tb, otb)):
        dst[...] = src[...]
    for copy in copies:
        copy.wait()


def on_device(pu, pd, pn, pb, mu, md, mn, mb, hu, hd, hn, hb):
    n = lax.axis_size("batch")
    size, width = pu.shape[1:]
    w = size // n
    count = 2 * SUBS
    line = lambda v: v.reshape(1, -1)
    shape = jax.ShapeDtypeStruct
    vmem = pl.BlockSpec(memory_space=pltpu.VMEM)
    hbm = pl.BlockSpec(memory_space=pltpu.HBM)
    dma = pltpu.SemaphoreType.DMA
    whole, share = (size, width), (w, width)
    row, part = (1, size), (1, w)
    owned = (shape(share, f32), shape(share, f32), shape(part, f32), shape(part, f32))
    results = pl.pallas_call(
        functools.partial(line_kernel, n, n ** (-0.5)),
        out_shape=(
            shape(whole, bf16), shape(whole, bf16), shape(row, f32), shape(row, f32),
            *owned, *owned,
        ),
        in_specs=(hbm,) * 12,
        out_specs=(vmem,) * 12,
        scratch_shapes=[
            pltpu.VMEM(whole, f32),
            pltpu.VMEM(whole, f32),
            *[pltpu.VMEM(share, f32)] * 4,
            *[pltpu.VMEM(row, f32)] * 2,
            *[pltpu.VMEM(part, f32)] * 4,
            pltpu.VMEM((2, *whole), bf16),
            pltpu.VMEM((2, 2, *whole), bf16),
            pltpu.VMEM((w // SUBS, width), f32),
            *[pltpu.VMEM((n, 2, w), f32)] * 3,
            dma((SUBS * n + 11,)),
            *[dma((2, count, n))] * 4,
            *[dma((2, n))] * 2,
        ],
        compiler_params=pltpu.CompilerParams(
            collective_id=0, has_side_effects=True, vmem_limit_bytes=MOST
        ),
    )(pu, pd, pn, pb, mu, md.T, line(mn), line(mb), hu, hd.T, line(hn), line(hb))
    cu, cd, cn, cb, su, sd, sn, sb, tu, td, tn, tb = pl.pallas_call(
        write_kernel,
        out_shape=(
            shape(whole, bf16), shape(whole, bf16), shape(row, bf16), shape(row, bf16),
            *owned, *owned,
        ),
        in_specs=(vmem,) * 12,
        out_specs=(hbm, hbm, vmem, vmem) * 3,
        scratch_shapes=[pltpu.VMEM(whole, bf16), dma((8,))],
        compiler_params=pltpu.CompilerParams(vmem_limit_bytes=MOST),
    )(*results)
    flat = lambda v: v.reshape(-1)
    return (
        cu, cd, flat(cn), flat(cb),
        su, sd.T, flat(sn), flat(sb),
        tu, td.T, flat(tn), flat(tb),
    )


def solution(mesh):
    own = (
        P(("shift", "batch"), "cols"),
        P(("shift", "cols"), "batch"),
        P(("shift", "batch")),
        P(("shift", "batch")),
    )
    return jax.shard_map(
        on_device,
        mesh=mesh,
        in_specs=(
            P(("shift", "batch"), None, "cols"),
            P(("shift", "batch"), "cols", None),
            P(("shift", "batch"), None),
            P(("shift", "batch"), None),
            *own,
            *own,
        ),
        out_specs=(
            P("shift", "cols"),
            P(("shift", "cols"), None),
            P("shift"),
            P("shift"),
            *own,
            *own,
        ),
        check_vma=False,
    )
```

```python
import functools

import jax
import jax.numpy as jnp
from jax import lax
from jax.experimental import pallas as pl
from jax.experimental.pallas import tpu as pltpu
from jax.sharding import PartitionSpec as P

learn_rate = 0.1
hold_rate = 0.8
bf16, f32 = jnp.bfloat16, jnp.float32
MESH = pl.DeviceIdType.MESH
RIGHT, LEFT = 0, 1
SUBS = 3
SKEW = 2
MOST = 67043328


def line_kernel(
    n, rate,
    pu, pd, pn, pb, mu, md, mn, mb, hu, hd, hn, hb,
    cu, cd, cn, cb, su, sd, sn, sb, tu, td, tn, tb,
    vpu, vpd, vmu, vmd, vhu, vhd, vpn, vpb, vmn, vmb, vhn, vhb,
    send, got, acc, vs, vr, vg,
    in_sem, rs_send, rs_recv, ag_send, ag_recv, vec_send, vec_recv,
):
    me = lax.axis_index("batch")
    size, width = vpu.shape
    w = size // n
    per = SUBS
    count = 2 * per
    r = w // per
    first, last = me == 0, me == n - 1
    toward = ({"batch": jnp.minimum(me + 1, n - 1)}, {"batch": jnp.maximum(me - 1, 0)})

    loads = {}

    def load(name, src, dst):
        copy = pltpu.make_async_copy(src, dst, in_sem.at[len(loads)])
        copy.start()
        loads[name] = copy

    def rows(q, j):
        if isinstance(j, int):
            return pl.ds(j * w + q % per * r, r)
        return pl.ds(pl.multiple_of(j * w + q % per * r, r), r)

    def part(q):
        return pl.ds(q % per * r, r)

    def load_up(q):
        for j in range(n):
            load((q, j), pu.at[0, rows(q, j), :], vpu.at[rows(q, j), :])

    load_up(0)
    load("down", pd.at[0], vpd)
    vectors = ((pn, vpn), (pb, vpb), (mn, vmn), (mb, vmb), (hn, vhn), (hb, vhb))
    for i, (src, dst) in enumerate(vectors):
        load(("vector", i), src, dst)
    load("mu", mu, vmu)
    load("hu", hu, vhu)
    for q in range(1, per):
        load_up(q)
    load("md", md, vmd)
    load("hd", hd, vhd)

    def at(d):
        return lax.rem(me + d + n, n)

    barrier = pltpu.get_barrier_semaphore()
    for d in range(1, n):
        pl.semaphore_signal(barrier, inc=1, device_id={"batch": at(d)}, device_id_type=MESH)

    def pack(q):
        if q < per:
            for j in range(n):
                loads[q, j].wait()
                send[0, rows(q, j), :] = vpu[rows(q, j), :].astype(bf16)
        elif q == per:
            loads["down"].wait()
            strip = width // 3
            for i in range(3):
                cut = slice(i * strip, (i + 1) * strip)
                send[1, :, cut] = vpd[cut, :].T.astype(bf16)

    def scatter(side, q, j):
        here = (q // per, rows(q, j))
        return pltpu.make_async_remote_copy(
            src_ref=send.at[here],
            dst_ref=got.at[(side, *here)],
            send_sem=rs_send.at[side, q, j],
            recv_sem=rs_recv.at[side, q, j],
            device_id=toward[side],
            device_id_type=MESH,
        )

    def gather(side, q, j):
        out = (cu, cd)[q // per].at[rows(q, j)]
        return pltpu.make_async_remote_copy(
            src_ref=out,
            dst_ref=out,
            send_sem=ag_send.at[side, q, j],
            recv_sem=ag_recv.at[side, q, j],
            device_id=toward[side],
            device_id_type=MESH,
        )

    def vector(phase, d, src, dst):
        return pltpu.make_async_remote_copy(
            src_ref=src,
            dst_ref=dst,
            send_sem=vec_send.at[phase, d],
            recv_sem=vec_recv.at[phase, d],
            device_id={"batch": at(d)},
            device_id_type=MESH,
        )

    def add(side, q, j):
        here = (q // per, rows(q, j))
        send[here] = (send[here].astype(f32) + got[(side, *here)].astype(f32)).astype(bf16)

    def start_ends(q):
        @pl.when(first)
        def _():
            for j in range(n - 1, 0, -1):
                scatter(RIGHT, q, j).start()

        @pl.when(last)
        def _():
            for j in range(n - 1):
                scatter(LEFT, q, j).start()

    def reduce(side, q, i):
        blocks = range(n - 1, i - 1, -1) if side == RIGHT else range(i + 1)
        for j in blocks:
            scatter(side, q, j).wait_recv()
            if j != i:
                add(side, q, j)
                scatter(side, q, j).start()

    def update(q):
        m, own, cut = q // per, rows(q, me), part(q)
        acc[...] = send[m, own].astype(f32)

        @pl.when(me > 0)
        def _():
            acc[...] += got[RIGHT, m, own].astype(f32)

        @pl.when(me < n - 1)
        def _():
            acc[...] += got[LEFT, m, own].astype(f32)

        state = hold_rate * (vhu, vhd)[m][cut, :] + acc[...] * rate
        stepped = (vmu, vmd)[m][cut, :] - learn_rate * state
        (cu, cd)[m][own, :] = stepped.astype(bf16)

        @pl.when(me < n - 1)
        def _():
            gather(RIGHT, q, me).start()

        @pl.when(me > 0)
        def _():
            gather(LEFT, q, me).start()

        (tu, td)[m][cut, :] = state
        (su, sd)[m][cut, :] = stepped

    def forward(side, q, i, j):
        gather(side, q, j).wait_recv()
        if i != (n - 1 if side == RIGHT else 0):
            gather(side, q, j).start()

    def hop(q, d):
        for i in range(n):
            tasks = []
            if i > 0 and d == SKEW * i:
                tasks.append(functools.partial(reduce, RIGHT, q, i))
            if i < n - 1 and d == SKEW * (n - 1 - i):
                tasks.append(functools.partial(reduce, LEFT, q, i))
            if d == SKEW * max(i, n - 1 - i):
                tasks.append(functools.partial(update, q))
            for j in range(n):
                if j != i and d == SKEW * (max(j, n - 1 - j) + abs(i - j)):
                    tasks.append(functools.partial(forward, RIGHT if j < i else LEFT, q, i, j))
            if tasks:
                @pl.when(me == i)
                def _():
                    for task in tasks:
                        task()

    pack(0)
    pl.semaphore_wait(barrier, n - 1)
    start_ends(0)
    for i in range(len(vectors)):
        loads["vector", i].wait()
    for k in range(n):
        vs[k, 0:1, :] = vpn[:, k * w : (k + 1) * w]
        vs[k, 1:2, :] = vpb[:, k * w : (k + 1) * w]
    for d in range(1, n):
        vector(0, d, vs.at[at(d)], vr.at[d]).start()

    for t in range(1, count + SKEW * (2 * n - 2)):
        if t < count:
            pack(t)
            start_ends(t)
        if t == 1:
            for name in ("mu", "hu", "md", "hd"):
                loads[name].wait()
        for q in range(count):
            hop(q, t - q)
        if t == 2:
            total = vs[me]
            for d in range(1, n):
                vector(0, d, vs.at[at(d)], vr.at[d]).wait_recv()
                total = total + vr[d]
            for i, (m, h, s, o) in enumerate(((vmn, vhn, tn, sn), (vmb, vhb, tb, sb))):
                state = hold_rate * h[...] + total[i : i + 1] * rate
                stepped = m[...] - learn_rate * state
                s[...] = state
                o[...] = stepped
                vg[me, i : i + 1, :] = stepped
            for d in range(1, n):
                vector(1, d, vg.at[me], vg.at[me]).start()
        if t == 3:
            for e in range(1, n):
                vector(1, e, vg.at[at(-e)], vg.at[at(-e)]).wait_recv()
            for k in range(n):
                cn[:, k * w : (k + 1) * w] = vg[k, 0:1, :]
                cb[:, k * w : (k + 1) * w] = vg[k, 1:2, :]

    for q in range(count):
        for j in range(n):
            @pl.when(me < j)
            def _():
                scatter(RIGHT, q, j).wait_send()

            @pl.when(me > j)
            def _():
                scatter(LEFT, q, j).wait_send()

            @pl.when(jnp.logical_and(me >= j, me < n - 1))
            def _():
                gather(RIGHT, q, j).wait_send()

            @pl.when(jnp.logical_and(me <= j, me > 0))
            def _():
                gather(LEFT, q, j).wait_send()
    for d in range(1, n):
        vector(0, d, vs.at[at(d)], vr.at[d]).wait_send()
        vector(1, d, vg.at[me], vg.at[me]).wait_send()


def write_kernel(
    cu, cd, cn, cb, su, sd, sn, sb, tu, td, tn, tb,
    ocu, ocd, ocn, ocb, osu, osd, osn, osb, otu, otd, otn, otb,
    vcd, sem,
):
    copies = [
        pltpu.make_async_copy(src, dst, sem.at[i])
        for i, (src, dst) in enumerate(((cu, ocu), (su, osu), (sd, osd), (tu, otu), (td, otd)))
    ]
    for copy in copies:
        copy.start()
    rows = vcd.shape[0]
    strip = rows // 3
    for i in range(3):
        r = slice(i * strip, (i + 1) * strip)
        vcd[r, :] = cd[:, r].astype(f32).T.astype(bf16)
        copies.append(pltpu.make_async_copy(vcd.at[r, :], ocd.at[r, :], sem.at[5 + i]))
        copies[-1].start()
    ocn[...] = cn[...]
    ocb[...] = cb[...]
    for src, dst in ((sn, osn), (sb, osb), (tn, otn), (tb, otb)):
        dst[...] = src[...]
    for copy in copies:
        copy.wait()


def on_device(pu, pd, pn, pb, mu, md, mn, mb, hu, hd, hn, hb):
    n = lax.axis_size("batch")
    size, width = pu.shape[1:]
    w = size // n
    count = 2 * SUBS
    line = lambda v: v.reshape(1, -1)
    shape = jax.ShapeDtypeStruct
    vmem = pl.BlockSpec(memory_space=pltpu.VMEM)
    hbm = pl.BlockSpec(memory_space=pltpu.HBM)
    dma = pltpu.SemaphoreType.DMA
    whole, share = (size, width), (w, width)
    row, part = (1, size), (1, w)
    owned = (shape(share, f32), shape(share, f32), shape(part, f32), shape(part, f32))
    results = pl.pallas_call(
        functools.partial(line_kernel, n, n ** (-0.5)),
        out_shape=(
            shape(whole, bf16), shape(whole, bf16), shape(row, f32), shape(row, f32),
            *owned, *owned,
        ),
        in_specs=(hbm,) * 12,
        out_specs=(vmem,) * 12,
        scratch_shapes=[
            pltpu.VMEM(whole, f32),
            pltpu.VMEM(whole, f32),
            *[pltpu.VMEM(share, f32)] * 4,
            *[pltpu.VMEM(row, f32)] * 2,
            *[pltpu.VMEM(part, f32)] * 4,
            pltpu.VMEM((2, *whole), bf16),
            pltpu.VMEM((2, 2, *whole), bf16),
            pltpu.VMEM((w // SUBS, width), f32),
            *[pltpu.VMEM((n, 2, w), f32)] * 3,
            dma((SUBS * n + 11,)),
            *[dma((2, count, n))] * 4,
            *[dma((2, n))] * 2,
        ],
        compiler_params=pltpu.CompilerParams(
            collective_id=0, has_side_effects=True, vmem_limit_bytes=MOST
        ),
    )(pu, pd, pn, pb, mu, md.T, line(mn), line(mb), hu, hd.T, line(hn), line(hb))
    cu, cd, cn, cb, su, sd, sn, sb, tu, td, tn, tb = pl.pallas_call(
        write_kernel,
        out_shape=(
            shape(whole, bf16), shape(whole, bf16), shape(row, f32), shape(row, f32),
            *owned, *owned,
        ),
        in_specs=(vmem,) * 12,
        out_specs=(hbm, hbm, vmem, vmem) * 3,
        scratch_shapes=[pltpu.VMEM(whole, bf16), dma((8,))],
        compiler_params=pltpu.CompilerParams(vmem_limit_bytes=MOST),
    )(*results)
    flat = lambda v: v.reshape(-1)
    return (
        cu, cd, flat(cn).astype(bf16), flat(cb).astype(bf16),
        su, sd.T, flat(sn), flat(sb),
        tu, td.T, flat(tn), flat(tb),
    )


def solution(mesh):
    own = (
        P(("shift", "batch"), "cols"),
        P(("shift", "cols"), "batch"),
        P(("shift", "batch")),
        P(("shift", "batch")),
    )
    return jax.shard_map(
        on_device,
        mesh=mesh,
        in_specs=(
            P(("shift", "batch"), None, "cols"),
            P(("shift", "batch"), "cols", None),
            P(("shift", "batch"), None),
            P(("shift", "batch"), None),
            *own,
            *own,
        ),
        out_specs=(
            P("shift", "cols"),
            P(("shift", "cols"), None),
            P("shift"),
            P("shift"),
            *own,
            *own,
        ),
        check_vma=False,
    )
```
